32 devices in a mesh: section: 4 (over y, x), dp: 8 (over z, core).
Axes of the slice: x: 2, y: 2, z: 4, core: 2. Of those that a mesh axis runs over, the one named last changes fastest.
Arguments:
- inputs: bfloat16 [8, 128, 16384], P(None, None, 'dp'), may hold values from -6 to 6
- cotangent: bfloat16 [4, 8, 128, 1024], P('section'), may hold values from -0.5 to 0.5
- norm_gain: bfloat16 [4, 16384], P('section', 'dp'), may hold values from 0.099609375 to 1.8984375
- value_weight: bfloat16 [4, 16384, 1024], P('section', 'dp'), may hold values from -0.046875 to 0.046875
- output_weight: bfloat16 [4, 1024, 16384], P('section', None, 'dp'), may hold values from -0.1875 to 0.1875
- left_old: float32 [4, 16, 1024, 1024], P('section', 'dp'), may hold values from -0.4 to 2.4, as said below
- right_old: float32 [4, 1024, 1024], P('section', 'dp'), may hold values from -0.4 to 2.4, as said below
Outputs:
- section_outputs: bfloat16 [4, 8, 128, 16384], P('section', None, None, 'dp')
- left_stats: float32 [4, 16, 1024, 1024], P('section', 'dp')
- right_stats: float32 [4, 1024, 1024], P('section', 'dp')
The draws below stay inside these ranges and needn't reach their ends.
Inputs may be any that keep to these rules, and one draw needn't show every extreme that they name: `left_old`: symmetric in its last two dimensions. `right_old`: symmetric in its last two dimensions.
All inputs are finite; a program needn't handle non-finite values.
Results may differ from the reference program's by a relative error of at most 0.015.
Values may be sent and summed in bfloat16 or wider, within the bound.
A program may use at most 128 MiB of HBM per device.

```python
import jax
import jax.numpy as jnp
from jax import lax

D = 16384
KV = 1024
BLOCK = 1024
MICRO = 8
MB = 128
SECTIONS = 4
NB = 16
N_SECTION = 4


def symmetric(key, leading, order):
    key_noise, key_diag = jax.random.split(key)
    noise_part = jnp.clip(jax.random.normal(key_noise, leading + (order, order), jnp.float32), -4.0, 4.0) * 0.05
    diagonal = jax.random.uniform(key_diag, leading + (order,), jnp.float32, 0.5, 2.0)
    return noise_part + jnp.swapaxes(noise_part, -1, -2) + diagonal[..., None] * jnp.eye(order, dtype=jnp.float32)


def draw_left_old(key, part):
    return symmetric(jax.random.fold_in(key, 11), (SECTIONS, NB), BLOCK)


def draw_right_old(key, part):
    return symmetric(jax.random.fold_in(key, 23), (SECTIONS,), KV)


def block_scale(rng, dims, pieces, low, largest):
    factor_of = 1.0
    for dim, shards_of in pieces:
        heights = jax.random.uniform(jax.random.fold_in(jax.random.fold_in(rng, 6), dim), (shards_of,), jnp.float32, low / len(pieces), largest / len(pieces))
        factor_of = factor_of * jnp.repeat(jnp.exp(heights), dims[dim] // shards_of).reshape((-1,) + (1,) * (len(dims) - 1 - dim))
    return factor_of


def normal_values(stream_key, extent, spread, reach, cuts=(), kind=jnp.bfloat16):
    array = jax.random.normal(stream_key, extent, jnp.float32) * spread
    if len(cuts) > 0:
        array = block_scale(stream_key, extent, cuts, -0.22, 0.18) * array
    return jnp.clip(array, min=-reach, max=reach).astype(kind)


def setup_inputs(seed: int = 0) -> dict:
    keys = jax.random.split(jax.random.key(seed), 8)
    return {
        "inputs": normal_values(keys[0], (MICRO, MB, D), 1.0, 6.0, ((2, 8),)),
        "cotangent": normal_values(keys[1], (SECTIONS, MICRO, MB, KV), 0.08, 0.5, ((0, 4),)),
        "norm_gain": jnp.clip(1.0 + 0.18 * jax.random.normal(keys[2], (SECTIONS, D), jnp.float32), 0.099609375, 1.8984375).astype(jnp.bfloat16),
        "value_weight": normal_values(keys[3], (SECTIONS, D, KV), D ** -0.5, 0.046875, ((0, 4), (1, 8))),
        "output_weight": normal_values(keys[4], (SECTIONS, KV, D), KV ** -0.5, 0.1875, ((0, 4), (2, 8))),
        "left_old": draw_left_old(jax.random.fold_in(keys[7], 71), 0),
        "right_old": draw_right_old(jax.random.fold_in(keys[7], 71), 0),
    }


def reference(inputs, cotangent, norm_gain, value_weight, output_weight, left_old, right_old):
    micro_count, batch_rows, model_width = inputs.shape
    hidden_in = inputs.reshape(micro_count * batch_rows, model_width)
    outputs_all = []
    lefts_all = []
    rights_all = []
    for layer_index in range(N_SECTION):
        floats = hidden_in.astype(jnp.float32)
        scaled_in = (floats * norm_gain[layer_index].astype(jnp.float32)).astype(jnp.bfloat16)
        inv_rms = lax.rsqrt(lax.optimization_barrier(jnp.mean(floats * floats, axis=1)) + 0.25)
        products = jnp.dot(scaled_in, value_weight[layer_index], preferred_element_type=jnp.float32)
        values = (inv_rms[:, None] * products).astype(jnp.bfloat16)
        hidden_in = (floats + jnp.dot(values, output_weight[layer_index], preferred_element_type=jnp.float32)).astype(jnp.bfloat16)
        cotan_rows = cotangent[layer_index].reshape(micro_count * batch_rows, KV).astype(jnp.float32)
        weighted = (inv_rms[:, None] * cotan_rows).astype(jnp.bfloat16)
        gradient = jnp.dot(scaled_in.T, weighted, preferred_element_type=jnp.float32).astype(jnp.bfloat16)
        blocks = gradient.reshape(NB, BLOCK, KV).astype(jnp.float32)
        left_new = left_old[layer_index] + jnp.einsum('bik,bjk->bij', blocks, blocks, precision=lax.Precision.HIGHEST) / BLOCK
        right_new = right_old[layer_index] + jnp.dot(gradient.T, gradient, preferred_element_type=jnp.float32) / D
        outputs_all.append(hidden_in.reshape(micro_count, batch_rows, model_width))
        lefts_all.append(left_new)
        rights_all.append(right_new)
    return (jnp.stack(outputs_all), jnp.stack(lefts_all), jnp.stack(rights_all))
```

```python
import functools

import jax
import jax.numpy as jnp
from jax import lax
from jax.experimental import pallas as pl
from jax.experimental.pallas import tpu as pltpu
from jax.sharding import PartitionSpec as P

BLOCK = 1024
VMEM_BYTES = 46 * 1024 * 1024
MESH = pl.DeviceIdType.MESH
F32 = jnp.float32
BF16 = jnp.bfloat16


def relay_kernel(
    sections, dp, model_width,
    x_in, cot_in, gain, wv_in, wo_in, left_in, right_in,
    out, acc, right_out,
    grad, scaled, weighted, cot, wv, wo, right_own, right_send, right_recv,
    z_send, z_recv,
    xbuf, prod, csum, invs, sq, pair_send, pair_recv, rs_send, rs_recv, vals,
    send_sem, recv_sem, load_sem, right_sem, z_sem,
):
    chips = dp // 2
    micro, rows_all, cols = x_in.shape
    width = wv.shape[1]
    half = rows_all // 2
    rows = half // chips
    share = width // dp
    s = lax.axis_index("section")
    d = lax.axis_index("dp")
    z = d // 2
    c = lax.rem(d, 2)
    partner = z * 2 + (1 - c)

    def device(section, index):
        return (section, index)

    loads = [
        pltpu.make_async_copy(src, dst, load_sem.at[i])
        for i, (src, dst) in enumerate(((wv_in, wv), (cot_in, cot), (wo_in, wo), (right_in, right_out)))
    ]
    left_load = pltpu.make_async_copy(left_in, acc, load_sem.at[4])

    @pl.when(s == 0)
    def _():
        pltpu.make_async_copy(x_in.at[0], xbuf.at[0], recv_sem.at[0, 0]).start()

    for load in loads:
        load.start()

    @pl.when(s == 0)
    def _():
        @pl.loop(1, micro)
        def _(m):
            pltpu.make_async_copy(x_in.at[m], xbuf.at[m], recv_sem.at[0, m]).start()

    barrier = pltpu.get_barrier_semaphore()
    for j in range(1, dp):
        pl.semaphore_signal(barrier, inc=1, device_id=device(s, lax.rem(d + j, dp)), device_id_type=MESH)

    @pl.when(s > 0)
    def _():
        pl.semaphore_signal(barrier, inc=1, device_id=device(s - 1, d), device_id_type=MESH)

    @pl.when(s < sections - 1)
    def _():
        pl.semaphore_signal(barrier, inc=1, device_id=device(s + 1, d), device_id_type=MESH)

    pl.semaphore_wait(
        barrier, dp - 1 + jnp.minimum(s, 1) + jnp.minimum(sections - 1 - s, 1)
    )

    def send(src, dst, phase, m, section, index):
        pltpu.make_async_remote_copy(
            src_ref=src, dst_ref=dst,
            send_sem=send_sem.at[phase, m], recv_sem=recv_sem.at[phase, m],
            device_id=device(section, index), device_id_type=MESH,
        ).start()

    def wait_in(ref, phase, m):
        pltpu.make_async_copy(ref, ref, recv_sem.at[phase, m]).wait()

    def wait_out(ref, phase, m):
        pltpu.make_async_copy(ref, ref, send_sem.at[phase, m]).wait()

    def step_project(m):
        wait_in(xbuf.at[m], 0, m)
        total = jnp.zeros((rows_all, 128), F32)
        for k in range(cols // 128):
            piece = xbuf[m, :, k * 128:(k + 1) * 128].astype(F32)
            total = total + piece * piece
            scaled[m, :, k * 128:(k + 1) * 128] = (
                piece * gain[:, k * 128:(k + 1) * 128].astype(F32)
            ).astype(BF16)
        row = jnp.sum(total.T, axis=0, keepdims=True)
        sq[m, d] = jnp.broadcast_to(row, (8, rows_all))
        for j in range(1, dp):
            send(sq.at[m, d], sq.at[m, d], 1, m, s, lax.rem(d + j, dp))

        @pl.when(m == 0)
        def _():
            loads[0].wait()

        @pl.loop(0, width // 256)
        def _(n):
            at = pl.ds(pl.multiple_of(n * 256, 256), 256)
            prod[:, at] = jnp.dot(scaled[m], wv[:, at], preferred_element_type=F32)

        pair_send[m] = prod[pl.ds(pl.multiple_of((1 - c) * half, half), half), :].astype(BF16)
        send(pair_send.at[m], pair_recv.at[m], 2, m, s, partner)

    def step_forward(m):
        wait_in(vals.at[m, c, pl.ds(0, chips - 1)], 4, m)
        send(vals.at[m, c], vals.at[m, c], 5, m, s, partner)

    def step_scatter(m):
        wait_in(pair_recv.at[m], 2, m)
        csum[...] = prod[pl.ds(pl.multiple_of(c * half, half), half), :] + pair_recv[m].astype(F32)
        for j in range(1, chips):
            target = lax.rem(z + j, chips)
            rs_send[m, j - 1] = csum[pl.ds(pl.multiple_of(target * rows, rows), rows), :].astype(BF16)
            send(rs_send.at[m, j - 1], rs_recv.at[m, chips - 1 - j], 3, m, s, target * 2 + c)

    def step_output(m):
        wait_in(vals.at[m, 1 - c], 5, m)

        @pl.when(m == 0)
        def _():
            loads[2].wait()

        values = vals[m].reshape(rows_all, width)

        for side in range(2):
            @pl.loop(0, cols // 1024)
            def _(n):
                at = pl.ds(pl.multiple_of(side * (cols // 2) + n * 512, 512), 512)
                out[m, :, at] = (
                    xbuf[m, :, at].astype(F32)
                    + jnp.dot(values, wo[:, at], preferred_element_type=F32)
                ).astype(BF16)

            cut = pl.ds(side * (cols // 2), cols // 2)

            @pl.when(s < sections - 1)
            def _():
                send(out.at[m, :, cut], xbuf.at[m, :, cut], 0, m, s + 1, d)

    def step_values(m):
        wait_in(sq.at[m, pl.ds(0, dp - 1)], 1, m)
        total_sq = jnp.sum(sq[m], axis=0)
        inv = lax.rsqrt(total_sq / model_width + 0.25)
        invs[...] = jnp.broadcast_to(inv[0:1, :], (rows_all, rows_all)).T
        wait_in(rs_recv.at[m], 3, m)
        total = csum[pl.ds(pl.multiple_of(z * rows, rows), rows), :]
        for j in range(chips - 1):
            total = total + rs_recv[m, j].astype(F32)
        own = invs[pl.ds(pl.multiple_of(c * half + z * rows, rows), rows), 0:1]
        vals[m, c, z] = (own * total).astype(BF16)
        for j in range(1, chips):
            target = lax.rem(z + j, chips)
            send(vals.at[m, c, z], vals.at[m, c, z], 4, m, s, target * 2 + c)

        @pl.when(m == 0)
        def _():
            loads[1].wait()

        weighted[m] = (invs[:, 0:1] * cot[m].astype(F32)).astype(BF16)

    contract_rows = (((0,), (0,)), ((), ()))
    tile = 256
    group = max(1, 256 // rows_all)
    groups = micro // group

    def gradient_tile(pair, n):
        at = pl.ds(pl.multiple_of(n * tile, tile), tile)
        left = scaled[pl.ds(pair * group, group), :, at].reshape(group * rows_all, tile)
        right = weighted[pl.ds(pair * group, group)].reshape(group * rows_all, width)
        return at, lax.dot_general(left, right, contract_rows, preferred_element_type=F32)

    def step_gradient(t):
        pair = (t - group) // group
        side = lax.rem(t, group)
        tiles = cols // tile // group

        @pl.loop(0, tiles)
        def _(i):
            at, update = gradient_tile(pair, side * tiles + i)

            @pl.when(pair == 0)
            def _():
                acc[at, :] = update

            @pl.when(pair > 0)
            def _():
                acc[at, :] += update

    def step_last_gradient():
        @pl.loop(0, cols // tile)
        def _(n):
            at, update = gradient_tile(groups - 1, n)
            grad[at, :] = (acc[at, :] + update).astype(BF16)

    def right_product(j):
        target = lax.rem(z + j, chips)
        at = pl.ds(pl.multiple_of(target * 2 * share, 2 * share), 2 * share)

        @pl.loop(0, width // 256)
        def _(n):
            cut = pl.ds(pl.multiple_of(n * 256, 256), 256)
            product = lax.dot_general(
                grad[:, at], grad[:, cut], contract_rows, preferred_element_type=F32
            )
            right_own[j, 0, :, cut] = product[:share]
            right_own[j, 1, :, cut] = product[share:]

        right_send[j] = right_own[j, 1 - c].astype(BF16)
        pltpu.make_async_remote_copy(
            src_ref=right_send.at[j], dst_ref=right_recv.at[j],
            send_sem=right_sem.at[0, j], recv_sem=right_sem.at[1, j],
            device_id=device(s, partner), device_id_type=MESH,
        ).start()

    def right_scatter(j):
        pltpu.make_async_copy(right_recv.at[j], right_recv.at[j], right_sem.at[1, j]).wait()
        z_send[j - 1] = (right_own[j, c] + right_recv[j].astype(F32)).astype(BF16)
        pltpu.make_async_remote_copy(
            src_ref=z_send.at[j - 1], dst_ref=z_recv.at[chips - 1 - j],
            send_sem=z_sem.at[0, j - 1], recv_sem=z_sem.at[1, chips - 1 - j],
            device_id=device(s, lax.rem(z + j, chips) * 2 + c), device_id_type=MESH,
        ).start()

    def step_right():
        for j in range(1, chips):
            right_product(j)
            if j > 1:
                right_scatter(j - 1)
        right_product(0)
        right_scatter(chips - 1)

    def step_left():
        left_load.wait()
        for block in range(cols // BLOCK):
            @pl.loop(0, BLOCK // 256)
            def _(n):
                at = pl.ds(pl.multiple_of(block * BLOCK + n * 256, 256), 256)
                product = lax.dot_general(
                    grad[at, :], grad[block * BLOCK:(block + 1) * BLOCK, :],
                    (((1,), (1,)), ((), ())), preferred_element_type=F32,
                )
                acc[at, :] += product * (1.0 / BLOCK)

    def step_last_right():
        pltpu.make_async_copy(right_recv.at[0], right_recv.at[0], right_sem.at[1, 0]).wait()
        total = right_own[0, c] + right_recv[0].astype(F32)
        for j in range(chips - 1):
            pltpu.make_async_copy(z_recv.at[j], z_recv.at[j], z_sem.at[1, j]).wait()
            total = total + z_recv[j].astype(F32)
        loads[3].wait()
        right_out[...] += total * (1.0 / model_width)
        for j in range(chips):
            pltpu.make_async_copy(right_send.at[j], right_send.at[j], right_sem.at[0, j]).wait()
        for j in range(chips - 1):
            pltpu.make_async_copy(z_send.at[j], z_send.at[j], z_sem.at[0, j]).wait()

    @pl.loop(0, micro + 2)
    def _(t):
        @pl.when(t < micro)
        def _():
            step_project(t)

        @pl.when((t >= 1) & (t <= micro))
        def _():
            step_values(t - 1)

        @pl.when(t >= 2)
        def _():
            step_output(t - 2)

        @pl.when(t < micro)
        def _():
            step_scatter(t)

        @pl.when((t >= group) & (t < micro))
        def _():
            step_gradient(t)

        @pl.when((t >= 1) & (t <= micro))
        def _():
            step_forward(t - 1)

        @pl.when(t == micro)
        def _():
            step_last_gradient()

    left_load.start()
    step_right()
    step_left()
    step_last_right()

    @pl.loop(0, micro)
    def _(m):
        wait_out(sq.at[m, pl.ds(0, dp - 1)], 1, m)
        wait_out(pair_send.at[m], 2, m)
        wait_out(rs_send.at[m], 3, m)
        wait_out(vals.at[m, c, pl.ds(0, chips - 1)], 4, m)
        wait_out(vals.at[m, c], 5, m)

        @pl.when(s < sections - 1)
        def _():
            wait_out(out.at[m], 0, m)


def relay(sections, dp, x_in, cot, gain, wv, wo, left, right):
    micro, rows_all, cols = x_in.shape
    width = wv.shape[1]
    chips = dp // 2
    half = rows_all // 2
    rows = half // chips
    share = width // dp
    vmem = pl.BlockSpec(memory_space=pltpu.VMEM)
    anywhere = pl.BlockSpec(memory_space=pl.ANY)
    return pl.pallas_call(
        functools.partial(relay_kernel, sections, dp, cols * dp),
        out_shape=(
            pltpu.VMEM((micro, rows_all, cols), BF16),
            pltpu.VMEM((cols, width), F32),
            pltpu.VMEM((share, width), F32),
        ),
        in_specs=[anywhere, anywhere, vmem, anywhere, anywhere, anywhere, anywhere],
        out_specs=(vmem, vmem, vmem),
        scratch_shapes=[
            pltpu.VMEM((cols, width), BF16),
            pltpu.VMEM((micro, rows_all, cols), BF16),
            pltpu.VMEM((micro, rows_all, width), BF16),
            pltpu.VMEM((micro, rows_all, width), BF16),
            pltpu.VMEM((cols, width), BF16),
            pltpu.VMEM((width, cols), BF16),
            pltpu.VMEM((chips, 2, share, width), F32),
            pltpu.VMEM((chips, share, width), BF16),
            pltpu.VMEM((chips, share, width), BF16),
            pltpu.VMEM((chips - 1, share, width), BF16),
            pltpu.VMEM((chips - 1, share, width), BF16),
            pltpu.VMEM((micro, rows_all, cols), BF16),
            pltpu.VMEM((rows_all, width), F32),
            pltpu.VMEM((half, width), F32),
            pltpu.VMEM((rows_all, rows_all), F32),
            pltpu.VMEM((micro, dp, 8, rows_all), F32),
            pltpu.VMEM((micro, half, width), BF16),
            pltpu.VMEM((micro, half, width), BF16),
            pltpu.VMEM((micro, chips - 1, rows, width), BF16),
            pltpu.VMEM((micro, chips - 1, rows, width), BF16),
            pltpu.VMEM((micro, 2, chips, rows, width), BF16),
            pltpu.SemaphoreType.DMA((6, micro)),
            pltpu.SemaphoreType.DMA((6, micro)),
            pltpu.SemaphoreType.DMA((5,)),
            pltpu.SemaphoreType.DMA((2, chips)),
            pltpu.SemaphoreType.DMA((2, chips - 1)),
        ],
        compiler_params=pltpu.CompilerParams(
            collective_id=0, has_side_effects=True, vmem_limit_bytes=VMEM_BYTES
        ),
    )(x_in, cot, gain, wv, wo, left, right)


def on_device(inputs, cotangent, norm_gain, value_weight, output_weight, left_old, right_old):
    sections = lax.axis_size("section")
    dp = lax.axis_size("dp")
    micro, rows_all, cols = inputs.shape
    width = value_weight.shape[2]
    chips = dp // 2
    split = 2 if rows_all // dp >= 16 else 1
    chunked = (micro * split, rows_all // split)
    outputs, left_new, right_new = relay(
        sections, dp, inputs.reshape(chunked + (cols,)), cotangent[0].reshape(chunked + (width,)),
        norm_gain, value_weight[0], output_weight[0], left_old.reshape(cols, width), right_old[0],
    )
    outputs = outputs.reshape((1, micro, rows_all, cols))
    return (outputs, left_new.reshape(left_old.shape), right_new[None])


def solution(mesh):
    placed = (
        P(None, None, "dp"),
        P("section", None, None, None),
        P("section", "dp"),
        P("section", "dp", None),
        P("section", None, "dp"),
        P("section", "dp", None, None),
        P("section", "dp", None),
    )
    return jax.shard_map(
        on_device,
        mesh=mesh,
        in_specs=placed,
        out_specs=(
            P("section", None, None, "dp"),
            P("section", "dp", None, None),
            P("section", "dp", None),
        ),
        check_vma=False,
    )
```

```python
import functools

import jax
import jax.numpy as jnp
from jax import lax
from jax.experimental import pallas as pl
from jax.experimental.pallas import tpu as pltpu
from jax.sharding import PartitionSpec as P

BLOCK = 1024
VMEM_BYTES = 46 * 1024 * 1024
MESH = pl.DeviceIdType.MESH
F32 = jnp.float32
BF16 = jnp.bfloat16


def relay_kernel(
    sections, dp, model_width,
    x_in, cot_in, gain, wv_in, wo_in, left_in, right_in,
    out, acc, right_out,
    grad, scaled, weighted, cot, wv, wo, right_own, right_send, right_recv,
    z_send, z_recv, help_in, help_recv, help_send, help_back,
    xbuf, prod, csum, invs, sq, pair_send, pair_recv, rs_send, rs_recv, vals,
    send_sem, recv_sem, load_sem, right_sem, z_sem, help_sem, back_sem,
):
    chips = dp // 2
    micro, rows_all, cols = x_in.shape
    width = wv.shape[1]
    half = rows_all // 2
    rows = half // chips
    share = width // dp
    s = lax.axis_index("section")
    d = lax.axis_index("dp")
    z = d // 2
    c = lax.rem(d, 2)
    partner = z * 2 + (1 - c)
    last = sections - 1
    helpers = (last ^ 2, last ^ 3) if sections % 4 == 0 else ()
    own_cols = width // 2 if helpers else width
    slice_cols = (width - own_cols) // max(1, len(helpers))

    def device(section, index):
        return (section, index)

    loads = [
        pltpu.make_async_copy(src, dst, load_sem.at[i])
        for i, (src, dst) in enumerate(((wv_in, wv), (cot_in, cot), (wo_in, wo), (right_in, right_out)))
    ]
    left_load = pltpu.make_async_copy(left_in, acc, load_sem.at[4])

    @pl.when(s == 0)
    def _():
        pltpu.make_async_copy(x_in.at[0], xbuf.at[0], recv_sem.at[0, 0]).start()

    loads[0].start()

    @pl.when(s == 0)
    def _():
        @pl.loop(1, micro)
        def _(m):
            pltpu.make_async_copy(x_in.at[m], xbuf.at[m], recv_sem.at[0, m]).start()

    barrier = pltpu.get_barrier_semaphore()
    for j in range(1, dp):
        pl.semaphore_signal(barrier, inc=1, device_id=device(s, lax.rem(d + j, dp)), device_id_type=MESH)

    @pl.when(s > 0)
    def _():
        pl.semaphore_signal(barrier, inc=1, device_id=device(s - 1, d), device_id_type=MESH)

    @pl.when(s < sections - 1)
    def _():
        pl.semaphore_signal(barrier, inc=1, device_id=device(s + 1, d), device_id_type=MESH)

    greeted = dp - 1 + jnp.minimum(s, 1) + jnp.minimum(sections - 1 - s, 1)
    for h in helpers:
        for there, here in ((last, h), (h, last)):
            @pl.when(s == here)
            def _():
                pl.semaphore_signal(barrier, inc=1, device_id=device(there, d), device_id_type=MESH)

            greeted = greeted + jnp.where(s == here, 1, 0)
    pl.semaphore_wait(barrier, greeted)

    def send(src, dst, phase, m, section, index):
        pltpu.make_async_remote_copy(
            src_ref=src, dst_ref=dst,
            send_sem=send_sem.at[phase, m], recv_sem=recv_sem.at[phase, m],
            device_id=device(section, index), device_id_type=MESH,
        ).start()

    def wait_in(ref, phase, m):
        pltpu.make_async_copy(ref, ref, recv_sem.at[phase, m]).wait()

    def wait_out(ref, phase, m):
        pltpu.make_async_copy(ref, ref, send_sem.at[phase, m]).wait()

    def step_project(m):
        wait_in(xbuf.at[m], 0, m)
        total = jnp.zeros((rows_all, 128), F32)
        for k in range(cols // 128):
            piece = xbuf[m, :, k * 128:(k + 1) * 128].astype(F32)
            total = total + piece * piece
            scaled[m, :, k * 128:(k + 1) * 128] = (
                piece * gain[:, k * 128:(k + 1) * 128].astype(F32)
            ).astype(BF16)
        row = jnp.sum(total.T, axis=0, keepdims=True)
        sq[m, d] = jnp.broadcast_to(row, (8, rows_all))
        for j in range(1, dp):
            send(sq.at[m, d], sq.at[m, d], 1, m, s, lax.rem(d + j, dp))

        @pl.when(m == 0)
        def _():
            loads[0].wait()
            for load in loads[1:]:
                load.start()

        prod[...] = jnp.dot(scaled[m], wv[...], preferred_element_type=F32)

        pair_send[m] = prod[pl.ds(pl.multiple_of((1 - c) * half, half), half), :].astype(BF16)
        send(pair_send.at[m], pair_recv.at[m], 2, m, s, partner)

    def step_forward(m):
        wait_in(vals.at[m, c, pl.ds(0, chips - 1)], 4, m)
        send(vals.at[m, c], vals.at[m, c], 5, m, s, partner)

    def step_scatter(m):
        wait_in(pair_recv.at[m], 2, m)
        csum[...] = prod[pl.ds(pl.multiple_of(c * half, half), half), :] + pair_recv[m].astype(F32)
        for j in range(1, chips):
            target = lax.rem(z + j, chips)
            rs_send[m, j - 1] = csum[pl.ds(pl.multiple_of(target * rows, rows), rows), :].astype(BF16)
            send(rs_send.at[m, j - 1], rs_recv.at[m, chips - 1 - j], 3, m, s, target * 2 + c)

    def step_output(m):
        wait_in(vals.at[m, 1 - c], 5, m)

        @pl.when(m == 0)
        def _():
            loads[2].wait()

        values = vals[m].reshape(rows_all, width)

        for side in range(4):
            @pl.loop(0, cols // 2048)
            def _(n):
                at = pl.ds(pl.multiple_of(side * (cols // 4) + n * 512, 512), 512)
                out[m, :, at] = (
                    xbuf[m, :, at].astype(F32)
                    + jnp.dot(values, wo[:, at], preferred_element_type=F32)
                ).astype(BF16)

            cut = pl.ds(side * (cols // 4), cols // 4)

            @pl.when(s < sections - 1)
            def _():
                send(out.at[m, :, cut], xbuf.at[m, :, cut], 0, m, s + 1, d)

    def step_weigh(m):
        wait_in(sq.at[m, pl.ds(0, dp - 1)], 1, m)
        total_sq = jnp.sum(sq[m], axis=0)
        inv = lax.rsqrt(total_sq / model_width + 0.25)
        invs[...] = jnp.broadcast_to(inv[0:1, :], (rows_all, rows_all)).T

        @pl.when(m == 0)
        def _():
            loads[1].wait()

        weighted[m] = (invs[:, 0:1] * cot[m].astype(F32)).astype(BF16)

    def step_values(m):
        wait_in(rs_recv.at[m], 3, m)
        total = csum[pl.ds(pl.multiple_of(z * rows, rows), rows), :]
        for j in range(chips - 1):
            total = total + rs_recv[m, j].astype(F32)
        own = invs[pl.ds(pl.multiple_of(c * half + z * rows, rows), rows), 0:1]
        vals[m, c, z] = (own * total).astype(BF16)
        for j in range(1, chips):
            target = lax.rem(z + j, chips)
            send(vals.at[m, c, z], vals.at[m, c, z], 4, m, s, target * 2 + c)

    contract_rows = (((0,), (0,)), ((), ()))
    tile = 256
    group = max(1, 256 // rows_all)
    groups = micro // group

    def gradient_tile(pair, n):
        at = pl.ds(pl.multiple_of(n * tile, tile), tile)
        left = scaled[pl.ds(pair * group, group), :, at].reshape(group * rows_all, tile)
        right = weighted[pl.ds(pair * group, group)].reshape(group * rows_all, width)
        return at, lax.dot_general(left, right, contract_rows, preferred_element_type=F32)

    def step_gradient(t):
        pair = (t - group) // group
        side = lax.rem(t, group)
        tiles = cols // tile // group

        @pl.loop(0, tiles)
        def _(i):
            at, update = gradient_tile(pair, side * tiles + i)

            @pl.when(pair == 0)
            def _():
                acc[at, :] = update

            @pl.when(pair > 0)
            def _():
                acc[at, :] += update

    def step_last_gradient():
        @pl.loop(0, cols // tile)
        def _(n):
            at, update = gradient_tile(groups - 1, n)
            grad[at, :] = (acc[at, :] + update).astype(BF16)

    def right_product(j):
        target = lax.rem(z + j, chips)
        at = pl.ds(pl.multiple_of(target * 2 * share, 2 * share), 2 * share)

        product = lax.dot_general(
            grad[:, at], grad[...], contract_rows, preferred_element_type=F32
        )
        right_own[j] = product.reshape(2, share, width)
        right_send[j] = right_own[j, 1 - c].astype(BF16)
        pltpu.make_async_remote_copy(
            src_ref=right_send.at[j], dst_ref=right_recv.at[j],
            send_sem=right_sem.at[0, j], recv_sem=right_sem.at[1, j],
            device_id=device(s, partner), device_id_type=MESH,
        ).start()

    def right_scatter(j):
        pltpu.make_async_copy(right_recv.at[j], right_recv.at[j], right_sem.at[1, j]).wait()
        z_send[j - 1] = (right_own[j, c] + right_recv[j].astype(F32)).astype(BF16)
        target = lax.rem(z + j, chips) * 2 + c
        slot = chips - 1 - j

        def scatter(cut, dst, part, recv, section, target=target):
            pltpu.make_async_remote_copy(
                src_ref=z_send.at[j - 1, :, cut], dst_ref=dst,
                send_sem=z_sem.at[0, j - 1, part], recv_sem=recv,
                device_id=device(section, target), device_id_type=MESH,
            ).start()

        own = pl.ds(0, own_cols)
        scatter(own, z_recv.at[slot, :, own], 0, z_sem.at[1, slot, 0], s)
        for i, h in enumerate(helpers):
            cut = pl.ds(own_cols + i * slice_cols, slice_cols)

            @pl.when(s == last)
            def _():
                scatter(cut, help_in.at[j - 1], 1 + i, help_sem.at[0, j - 1], h, d)

            @pl.when(s < last)
            def _():
                scatter(cut, z_recv.at[slot, :, cut], 1 + i, z_sem.at[1, slot, 1 + i], s)

    def step_right():
        for j in range(1, chips):
            right_product(j)
            if j > 1:
                right_scatter(j - 1)
        right_product(0)
        right_scatter(chips - 1)

    def step_left():
        left_load.wait()
        for block in range(cols // BLOCK):
            @pl.loop(0, BLOCK // 256)
            def _(n):
                at = pl.ds(pl.multiple_of(block * BLOCK + n * 256, 256), 256)
                product = lax.dot_general(
                    grad[at, :], grad[block * BLOCK:(block + 1) * BLOCK, :],
                    (((1,), (1,)), ((), ())), preferred_element_type=F32,
                )
                acc[at, :] += product * (1.0 / BLOCK)

    def step_last_right():
        pltpu.make_async_copy(right_recv.at[0], right_recv.at[0], right_sem.at[1, 0]).wait()
        loads[3].wait()
        scale = 1.0 / model_width

        def gather(cut, part):
            total = right_own[0, c, :, cut] + right_recv[0, :, cut].astype(F32)
            for k in range(chips - 1):
                ref = z_recv.at[k, :, cut]
                pltpu.make_async_copy(ref, ref, z_sem.at[1, k, part]).wait()
                total = total + z_recv[k, :, cut].astype(F32)
            right_out[:, cut] += total * scale

        gather(pl.ds(0, own_cols), 0)
        for i, h in enumerate(helpers):
            cut = pl.ds(own_cols + i * slice_cols, slice_cols)

            @pl.when(s == last)
            def _():
                ref = help_back.at[i]
                pltpu.make_async_copy(ref, ref, back_sem.at[1, i]).wait()
                total = right_own[0, c, :, cut] + right_recv[0, :, cut].astype(F32)
                right_out[:, cut] += (total + help_back[i].astype(F32)) * scale

            @pl.when(s < last)
            def _():
                gather(cut, 1 + i)

        for j in range(chips):
            pltpu.make_async_copy(right_send.at[j], right_send.at[j], right_sem.at[0, j]).wait()
        for j in range(chips - 1):
            for part in range(1 + len(helpers)):
                ref = z_send.at[j, :, pl.ds(0, slice_cols if part else own_cols)]
                pltpu.make_async_copy(ref, ref, z_sem.at[0, j, part]).wait()

    def step_help():
        for i, h in enumerate(helpers):
            @pl.when(s == h)
            def _():
                for j in range(1, chips):
                    ref = help_in.at[j - 1]
                    pltpu.make_async_copy(ref, ref, help_sem.at[0, j - 1]).wait()
                    pltpu.make_async_remote_copy(
                        src_ref=ref, dst_ref=help_recv.at[chips - 1 - j],
                        send_sem=help_sem.at[2, j - 1], recv_sem=help_sem.at[1, chips - 1 - j],
                        device_id=device(s, lax.rem(z + j, chips) * 2 + c), device_id_type=MESH,
                    ).start()
                total = None
                for k in range(chips - 1):
                    ref = help_recv.at[k]
                    pltpu.make_async_copy(ref, ref, help_sem.at[1, k]).wait()
                    piece = help_recv[k].astype(F32)
                    total = piece if total is None else total + piece
                help_send[...] = total.astype(BF16)
                back = pltpu.make_async_remote_copy(
                    src_ref=help_send, dst_ref=help_back.at[i],
                    send_sem=back_sem.at[0, i], recv_sem=back_sem.at[1, i],
                    device_id=device(last, d), device_id_type=MESH,
                )
                back.start()
                for k in range(chips - 1):
                    ref = help_in.at[k]
                    pltpu.make_async_copy(ref, ref, help_sem.at[2, k]).wait()
                back.wait_send()

    @pl.when(s == 0)
    def _():
        @pl.loop(0, micro + 2)
        def _(t):
            @pl.when(t < micro)
            def _():
                step_project(t - 0)

            @pl.when(t >= 2)
            def _():
                step_forward(t - 2)

            @pl.when((t >= 1) & (t < micro + 1))
            def _():
                step_weigh(t - 1)

            @pl.when((t >= 1) & (t < micro + 1))
            def _():
                step_values(t - 1)

            @pl.when((t >= group) & (t < micro))
            def _():
                step_gradient(t)

            @pl.when(t == micro)
            def _():
                step_last_gradient()

            @pl.when(t < micro)
            def _():
                step_scatter(t - 0)

            @pl.when(t >= 2)
            def _():
                step_output(t - 2)


    @pl.when((s > 0) & (s < last))
    def _():
        @pl.loop(0, micro + 2)
        def _(t):
            @pl.when(t < micro)
            def _():
                step_project(t - 0)

            @pl.when((t >= 1) & (t < micro + 1))
            def _():
                step_weigh(t - 1)

            @pl.when((t >= 1) & (t < micro + 1))
            def _():
                step_values(t - 1)

            @pl.when(t >= 2)
            def _():
                step_output(t - 2)

            @pl.when(t < micro)
            def _():
                step_scatter(t - 0)

            @pl.when((t >= group) & (t < micro))
            def _():
                step_gradient(t)

            @pl.when(t == micro)
            def _():
                step_last_gradient()

            @pl.when((t >= 1) & (t < micro + 1))
            def _():
                step_forward(t - 1)


    @pl.when(s == last)
    def _():
        @pl.loop(0, micro + 2)
        def _(t):
            @pl.when(t < micro)
            def _():
                step_project(t - 0)

            @pl.when((t >= 1) & (t < micro))
            def _():
                step_weigh(t - 1)
                step_values(t - 1)

            @pl.when(t >= 2)
            def _():
                step_output(t - 2)

            @pl.when(t < micro)
            def _():
                step_scatter(t - 0)

            @pl.when((t >= group) & (t < micro))
            def _():
                step_gradient(t)

            @pl.when(t == micro - 1)
            def _():
                step_weigh(t)
                step_last_gradient()
                left_load.start()
                step_values(t)
                step_right()

            @pl.when((t >= 1) & (t < micro + 1))
            def _():
                step_forward(t - 1)


    @pl.when(s < last)
    def _():
        left_load.start()
        step_right()

    step_left()
    step_last_right()
    step_help()

    @pl.loop(0, micro)
    def _(m):
        wait_out(sq.at[m, pl.ds(0, dp - 1)], 1, m)
        wait_out(pair_send.at[m], 2, m)
        wait_out(rs_send.at[m], 3, m)
        wait_out(vals.at[m, c, pl.ds(0, chips - 1)], 4, m)
        wait_out(vals.at[m, c], 5, m)

        @pl.when(s < sections - 1)
        def _():
            wait_out(out.at[m], 0, m)


def relay(sections, dp, x_in, cot, gain, wv, wo, left, right):
    micro, rows_all, cols = x_in.shape
    width = wv.shape[1]
    chips = dp // 2
    half = rows_all // 2
    rows = half // chips
    share = width // dp
    vmem = pl.BlockSpec(memory_space=pltpu.VMEM)
    anywhere = pl.BlockSpec(memory_space=pl.ANY)
    return pl.pallas_call(
        functools.partial(relay_kernel, sections, dp, cols * dp),
        out_shape=(
            pltpu.VMEM((micro, rows_all, cols), BF16),
            pltpu.VMEM((cols, width), F32),
            pltpu.VMEM((share, width), F32),
        ),
        in_specs=[anywhere, anywhere, vmem, anywhere, anywhere, anywhere, anywhere],
        out_specs=(vmem, vmem, vmem),
        scratch_shapes=[
            pltpu.VMEM((cols, width), BF16),
            pltpu.VMEM((micro, rows_all, cols), BF16),
            pltpu.VMEM((micro, rows_all, width), BF16),
            pltpu.VMEM((micro, rows_all, width), BF16),
            pltpu.VMEM((cols, width), BF16),
            pltpu.VMEM((width, cols), BF16),
            pltpu.VMEM((chips, 2, share, width), F32),
            pltpu.VMEM((chips, share, width), BF16),
            pltpu.VMEM((chips, share, width), BF16),
            pltpu.VMEM((chips - 1, share, width), BF16),
            pltpu.VMEM((chips - 1, share, width), BF16),
            pltpu.VMEM((chips - 1, share, width // 4), BF16),
            pltpu.VMEM((chips - 1, share, width // 4), BF16),
            pltpu.VMEM((share, width // 4), BF16),
            pltpu.VMEM((2, share, width // 4), BF16),
            pltpu.VMEM((micro, rows_all, cols), BF16),
            pltpu.VMEM((rows_all, width), F32),
            pltpu.VMEM((half, width), F32),
            pltpu.VMEM((rows_all, rows_all), F32),
            pltpu.VMEM((micro, dp, 8, rows_all), F32),
            pltpu.VMEM((micro, half, width), BF16),
            pltpu.VMEM((micro, half, width), BF16),
            pltpu.VMEM((micro, chips - 1, rows, width), BF16),
            pltpu.VMEM((micro, chips - 1, rows, width), BF16),
            pltpu.VMEM((micro, 2, chips, rows, width), BF16),
            pltpu.SemaphoreType.DMA((6, micro)),
            pltpu.SemaphoreType.DMA((6, micro)),
            pltpu.SemaphoreType.DMA((5,)),
            pltpu.SemaphoreType.DMA((2, chips)),
            pltpu.SemaphoreType.DMA((2, chips - 1, 3)),
            pltpu.SemaphoreType.DMA((3, chips - 1)),
            pltpu.SemaphoreType.DMA((2, 2)),
        ],
        compiler_params=pltpu.CompilerParams(
            collective_id=0, has_side_effects=True, vmem_limit_bytes=VMEM_BYTES
        ),
    )(x_in, cot, gain, wv, wo, left, right)


def on_device(inputs, cotangent, norm_gain, value_weight, output_weight, left_old, right_old):
    sections = lax.axis_size("section")
    dp = lax.axis_size("dp")
    micro, rows_all, cols = inputs.shape
    width = value_weight.shape[2]
    chips = dp // 2
    split = 2 if rows_all // dp >= 16 else 1
    chunked = (micro * split, rows_all // split)
    outputs, left_new, right_new = relay(
        sections, dp, inputs.reshape(chunked + (cols,)), cotangent[0].reshape(chunked + (width,)),
        norm_gain, value_weight[0], output_weight[0], left_old.reshape(cols, width), right_old[0],
    )
    outputs = outputs.reshape((1, micro, rows_all, cols))
    return (outputs, left_new.reshape(left_old.shape), right_new[None])


def solution(mesh):
    placed = (
        P(None, None, "dp"),
        P("section", None, None, None),
        P("section", "dp"),
        P("section", "dp", None),
        P("section", None, "dp"),
        P("section", "dp", None, None),
        P("section", "dp", None),
    )
    return jax.shard_map(
        on_device,
        mesh=mesh,
        in_specs=placed,
        out_specs=(
            P("section", None, None, "dp"),
            P("section", "dp", None, None),
            P("section", "dp", None),
        ),
        check_vma=False,
    )
```

```python
import functools

import jax
import jax.numpy as jnp
from jax import lax
from jax.experimental import pallas as pl
from jax.experimental.pallas import tpu as pltpu
from jax.sharding import PartitionSpec as P

BLOCK = 1024
PIECES = 4
VMEM_BYTES = 46 * 1024 * 1024
MESH = pl.DeviceIdType.MESH
F32 = jnp.float32
BF16 = jnp.bfloat16


def owner_chips(chips):
    return (chips // 2 - 1, chips // 2) if chips >= 4 else tuple(range(chips))


def relay_kernel(
    sections, dp, model_width,
    x_in, cot_in, gain, wv_in, wo_in, left_in, right_in,
    out, acc, right_out,
    grad, scaled, weighted, cot, wv, wo, right_own, right_send, right_recv,
    z_send, z_recv, help_in, help_recv, help_send, help_back,
    xbuf, prod, csum, invs, sq, pair_send, pair_recv, rs_send, rs_recv, vals,
    send_sem, recv_sem, x_sem, load_sem, right_sem, z_sem, help_sem, back_sem,
):
    chips = dp // 2
    micro, rows_all, cols = x_in.shape
    width = wv.shape[1]
    half = rows_all // 2
    owners = owner_chips(chips)
    rows = half // len(owners)
    share = width // dp
    s = lax.axis_index("section")
    d = lax.axis_index("dp")
    z = d // 2
    c = lax.rem(d, 2)
    partner = z * 2 + (1 - c)
    last = sections - 1
    helpers = (last ^ 2, last ^ 3) if sections % 4 == 0 else ()
    own_cols = width // 2 if helpers else width
    slice_cols = (width - own_cols) // max(1, len(helpers))

    def device(section, index):
        return (section, index)

    piece = cols // PIECES

    def load_x(m):
        for p in range(PIECES):
            lanes = pl.ds(p * piece, piece)
            pltpu.make_async_copy(
                x_in.at[m, :, lanes], xbuf.at[m, :, lanes], x_sem.at[p, m]
            ).start()

    loads = [
        pltpu.make_async_copy(src, dst, load_sem.at[i])
        for i, (src, dst) in enumerate(((wv_in, wv), (cot_in, cot), (wo_in, wo), (right_in, right_out)))
    ]
    left_load = pltpu.make_async_copy(left_in, acc, load_sem.at[4])

    @pl.when(s == 0)
    def _():
        load_x(0)

    loads[0].start()

    @pl.when(s == 0)
    def _():
        @pl.loop(1, micro)
        def _(m):
            load_x(m)

    barrier = pltpu.get_barrier_semaphore()
    for j in range(1, dp):
        pl.semaphore_signal(barrier, inc=1, device_id=device(s, lax.rem(d + j, dp)), device_id_type=MESH)

    @pl.when(s > 0)
    def _():
        pl.semaphore_signal(barrier, inc=1, device_id=device(s - 1, d), device_id_type=MESH)

    @pl.when(s < sections - 1)
    def _():
        pl.semaphore_signal(barrier, inc=1, device_id=device(s + 1, d), device_id_type=MESH)

    greeted = dp - 1 + jnp.minimum(s, 1) + jnp.minimum(sections - 1 - s, 1)
    for h in helpers:
        for there, here in ((last, h), (h, last)):
            @pl.when(s == here)
            def _():
                pl.semaphore_signal(barrier, inc=1, device_id=device(there, d), device_id_type=MESH)

            greeted = greeted + jnp.where(s == here, 1, 0)

    pl.semaphore_wait(barrier, greeted)

    def send(src, dst, phase, m, section, index):
        pltpu.make_async_remote_copy(
            src_ref=src, dst_ref=dst,
            send_sem=send_sem.at[phase, m], recv_sem=recv_sem.at[phase, m],
            device_id=device(section, index), device_id_type=MESH,
        ).start()

    def wait_in(ref, phase, m):
        pltpu.make_async_copy(ref, ref, recv_sem.at[phase, m]).wait()

    def wait_out(ref, phase, m):
        pltpu.make_async_copy(ref, ref, send_sem.at[phase, m]).wait()

    def step_project(m):
        total = jnp.zeros((rows_all, 128), F32)
        for p in range(PIECES):
            lanes = pl.ds(p * piece, piece)
            ref = xbuf.at[m, :, lanes]
            pltpu.make_async_copy(ref, ref, x_sem.at[p, m]).wait()
            for k in range(p * piece // 128, (p + 1) * piece // 128):
                values = xbuf[m, :, k * 128:(k + 1) * 128].astype(F32)
                total = total + values * values
                scaled[m, :, k * 128:(k + 1) * 128] = (
                    values * gain[:, k * 128:(k + 1) * 128].astype(F32)
                ).astype(BF16)
            if p == PIECES - 1:
                row = jnp.sum(total.T, axis=0, keepdims=True)
                sq[m, d] = jnp.broadcast_to(row, (8, rows_all))
                for j in range(1, dp):
                    send(sq.at[m, d], sq.at[m, d], 1, m, s, lax.rem(d + j, dp))
            if p == 0:
                @pl.when(m == 0)
                def _():
                    loads[0].wait()
                    for load in loads[1:]:
                        load.start()
            product = jnp.dot(scaled[m, :, lanes], wv[lanes, :], preferred_element_type=F32)
            if p == 0:
                prod[...] = product
            else:
                prod[...] += product

        pair_send[m] = prod[pl.ds(pl.multiple_of((1 - c) * half, half), half), :].astype(BF16)
        send(pair_send.at[m], pair_recv.at[m], 2, m, s, partner)

    is_owner = functools.reduce(jnp.logical_or, [z == owner for owner in owners])

    def wait_values(wait, m):
        @pl.when(is_owner)
        def _():
            if len(owners) > 1:
                wait(vals.at[m, c, pl.ds(0, len(owners) - 1)], 4, m)

        @pl.when(jnp.logical_not(is_owner))
        def _():
            wait(vals.at[m, c], 4, m)

    def step_forward(m):
        wait_values(wait_in, m)
        send(vals.at[m, c], vals.at[m, c], 5, m, s, partner)

    def step_scatter(m):
        wait_in(pair_recv.at[m], 2, m)
        csum[...] = prod[pl.ds(pl.multiple_of(c * half, half), half), :] + pair_recv[m].astype(F32)
        for i, owner in enumerate(owners):
            @pl.when(z != owner)
            def _():
                rs_send[m, i] = csum[i * rows:(i + 1) * rows, :].astype(BF16)
                slot = lax.rem(z - owner + chips, chips) - 1
                send(rs_send.at[m, i], rs_recv.at[m, slot], 3, m, s, owner * 2 + c)

    def step_output(m):
        wait_in(vals.at[m, 1 - c], 5, m)

        @pl.when(m == 0)
        def _():
            loads[2].wait()

        values = vals[m].reshape(rows_all, width)

        for p in range(PIECES):
            lanes = pl.ds(p * piece, piece)
            out[m, :, lanes] = (
                xbuf[m, :, lanes].astype(F32)
                + jnp.dot(values, wo[:, lanes], preferred_element_type=F32)
            ).astype(BF16)

            @pl.when(s < sections - 1)
            def _():
                pltpu.make_async_remote_copy(
                    src_ref=out.at[m, :, lanes], dst_ref=xbuf.at[m, :, lanes],
                    send_sem=send_sem.at[0, m], recv_sem=x_sem.at[p, m],
                    device_id=device(s + 1, d), device_id_type=MESH,
                ).start()

    def step_weigh(m):
        wait_in(sq.at[m, pl.ds(0, dp - 1)], 1, m)
        total_sq = jnp.sum(sq[m], axis=0)
        inv = lax.rsqrt(total_sq / model_width + 0.25)
        invs[...] = jnp.broadcast_to(inv[0:1, :], (rows_all, rows_all)).T

        @pl.when(m == 0)
        def _():
            loads[1].wait()

        weighted[m] = (invs[:, 0:1] * cot[m].astype(F32)).astype(BF16)

    def step_values(m):
        for i, owner in enumerate(owners):
            @pl.when(z == owner)
            def _():
                wait_in(rs_recv.at[m], 3, m)
                total = csum[i * rows:(i + 1) * rows, :]
                for j in range(chips - 1):
                    total = total + rs_recv[m, j].astype(F32)
                own = invs[pl.ds(pl.multiple_of(c * half + i * rows, rows), rows), 0:1]
                vals[m, c, i] = (own * total).astype(BF16)
                for j in range(1, chips):
                    target = (owner + j) % chips
                    send(vals.at[m, c, i], vals.at[m, c, i], 4, m, s, target * 2 + c)

    contract_rows = (((0,), (0,)), ((), ()))
    group = max(1, 256 // rows_all)
    groups = micro // group

    def gradient_tile(pair, n, tile):
        at = pl.ds(pl.multiple_of(n * tile, tile), tile)
        left = scaled[pl.ds(pair * group, group), :, at].reshape(group * rows_all, tile)
        right = weighted[pl.ds(pair * group, group)].reshape(group * rows_all, width)
        return at, lax.dot_general(left, right, contract_rows, preferred_element_type=F32)

    def step_gradient(t):
        pair = (t - group) // group
        at, update = gradient_tile(pair, lax.rem(t, group), cols // group)

        @pl.when(pair == 0)
        def _():
            acc[at, :] = update

        @pl.when(pair > 0)
        def _():
            acc[at, :] += update

    def step_last_gradient():
        tile = cols // 2

        @pl.loop(0, 2)
        def _(n):
            at, update = gradient_tile(groups - 1, n, tile)
            grad[at, :] = (acc[at, :] + update).astype(BF16)

    def right_product(j):
        target = lax.rem(z + j, chips)
        at = pl.ds(pl.multiple_of(target * 2 * share, 2 * share), 2 * share)

        product = lax.dot_general(
            grad[:, at], grad[...], contract_rows, preferred_element_type=F32
        )
        right_own[j] = product.reshape(2, share, width)
        right_send[j] = right_own[j, 1 - c].astype(BF16)
        pltpu.make_async_remote_copy(
            src_ref=right_send.at[j], dst_ref=right_recv.at[j],
            send_sem=right_sem.at[0, j], recv_sem=right_sem.at[1, j],
            device_id=device(s, partner), device_id_type=MESH,
        ).start()

    def right_scatter(j):
        pltpu.make_async_copy(right_recv.at[j], right_recv.at[j], right_sem.at[1, j]).wait()
        z_send[j - 1] = (right_own[j, c] + right_recv[j].astype(F32)).astype(BF16)
        target = lax.rem(z + j, chips) * 2 + c
        slot = chips - 1 - j

        def scatter(cut, dst, part, recv, section, target=target):
            pltpu.make_async_remote_copy(
                src_ref=z_send.at[j - 1, :, cut], dst_ref=dst,
                send_sem=z_sem.at[0, j - 1, part], recv_sem=recv,
                device_id=device(section, target), device_id_type=MESH,
            ).start()

        own = pl.ds(0, own_cols)
        scatter(own, z_recv.at[slot, :, own], 0, z_sem.at[1, slot, 0], s)
        for i, h in enumerate(helpers):
            cut = pl.ds(own_cols + i * slice_cols, slice_cols)

            @pl.when(s == last)
            def _():
                scatter(cut, help_in.at[j - 1], 1 + i, help_sem.at[0, j - 1], h, d)

            @pl.when(s < last)
            def _():
                scatter(cut, z_recv.at[slot, :, cut], 1 + i, z_sem.at[1, slot, 1 + i], s)

    def step_right():
        for j in range(1, chips):
            right_product(j)
            if j > 1:
                right_scatter(j - 1)
        right_product(0)
        right_scatter(chips - 1)

    def step_left():
        left_load.wait()
        for block in range(cols // BLOCK):
            @pl.loop(0, BLOCK // 512)
            def _(n):
                at = pl.ds(pl.multiple_of(block * BLOCK + n * 512, 512), 512)
                product = lax.dot_general(
                    grad[at, :], grad[block * BLOCK:(block + 1) * BLOCK, :],
                    (((1,), (1,)), ((), ())), preferred_element_type=F32,
                )
                acc[at, :] += product * (1.0 / BLOCK)

    def step_last_right():
        pltpu.make_async_copy(right_recv.at[0], right_recv.at[0], right_sem.at[1, 0]).wait()
        loads[3].wait()
        scale = 1.0 / model_width

        def gather(cut, part):
            total = right_own[0, c, :, cut] + right_recv[0, :, cut].astype(F32)
            for k in range(chips - 1):
                ref = z_recv.at[k, :, cut]
                pltpu.make_async_copy(ref, ref, z_sem.at[1, k, part]).wait()
                total = total + z_recv[k, :, cut].astype(F32)
            right_out[:, cut] += total * scale

        gather(pl.ds(0, own_cols), 0)
        for i, h in enumerate(helpers):
            cut = pl.ds(own_cols + i * slice_cols, slice_cols)

            @pl.when(s == last)
            def _():
                ref = help_back.at[i]
                pltpu.make_async_copy(ref, ref, back_sem.at[1, i]).wait()
                total = right_own[0, c, :, cut] + right_recv[0, :, cut].astype(F32)
                right_out[:, cut] += (total + help_back[i].astype(F32)) * scale

            @pl.when(s < last)
            def _():
                gather(cut, 1 + i)

        for j in range(chips):
            pltpu.make_async_copy(right_send.at[j], right_send.at[j], right_sem.at[0, j]).wait()
        for j in range(chips - 1):
            for part in range(1 + len(helpers)):
                ref = z_send.at[j, :, pl.ds(0, slice_cols if part else own_cols)]
                pltpu.make_async_copy(ref, ref, z_sem.at[0, j, part]).wait()

    def step_help():
        for i, h in enumerate(helpers):
            @pl.when(s == h)
            def _():
                for j in range(1, chips):
                    ref = help_in.at[j - 1]
                    pltpu.make_async_copy(ref, ref, help_sem.at[0, j - 1]).wait()
                    pltpu.make_async_remote_copy(
                        src_ref=ref, dst_ref=help_recv.at[chips - 1 - j],
                        send_sem=help_sem.at[2, j - 1], recv_sem=help_sem.at[1, chips - 1 - j],
                        device_id=device(s, lax.rem(z + j, chips) * 2 + c), device_id_type=MESH,
                    ).start()
                total = None
                for k in range(chips - 1):
                    ref = help_recv.at[k]
                    pltpu.make_async_copy(ref, ref, help_sem.at[1, k]).wait()
                    piece = help_recv[k].astype(F32)
                    total = piece if total is None else total + piece
                help_send[...] = total.astype(BF16)
                back = pltpu.make_async_remote_copy(
                    src_ref=help_send, dst_ref=help_back.at[i],
                    send_sem=back_sem.at[0, i], recv_sem=back_sem.at[1, i],
                    device_id=device(last, d), device_id_type=MESH,
                )
                back.start()
                for k in range(chips - 1):
                    ref = help_in.at[k]
                    pltpu.make_async_copy(ref, ref, help_sem.at[2, k]).wait()
                back.wait_send()

    @pl.when(s == 0)
    def _():
        @pl.loop(0, micro + 2)
        def _(t):
            @pl.when(t < micro)
            def _():
                step_project(t - 0)

            @pl.when(t >= 2)
            def _():
                step_forward(t - 2)

            @pl.when((t >= 1) & (t < micro + 1))
            def _():
                step_weigh(t - 1)

            @pl.when((t >= 1) & (t < micro + 1))
            def _():
                step_values(t - 1)

            @pl.when((t >= group) & (t < micro))
            def _():
                step_gradient(t)

            @pl.when(t == micro)
            def _():
                step_last_gradient()

            @pl.when(t < micro)
            def _():
                step_scatter(t - 0)

            @pl.when(t >= 2)
            def _():
                step_output(t - 2)


    @pl.when((s > 0) & (s < last))
    def _():
        @pl.loop(0, micro + 2)
        def _(t):
            @pl.when(t < micro)
            def _():
                step_project(t - 0)

            @pl.when((t >= 1) & (t < micro + 1))
            def _():
                step_weigh(t - 1)

            @pl.when((t >= 1) & (t < micro + 1))
            def _():
                step_values(t - 1)

            @pl.when(t >= 2)
            def _():
                step_output(t - 2)

            @pl.when(t < micro)
            def _():
                step_scatter(t - 0)

            @pl.when((t >= group) & (t < micro))
            def _():
                step_gradient(t)

            @pl.when(t == micro)
            def _():
                step_last_gradient()

            @pl.when((t >= 1) & (t < micro + 1))
            def _():
                step_forward(t - 1)


    @pl.when(s == last)
    def _():
        @pl.loop(0, micro + 2)
        def _(t):
            @pl.when(t < micro)
            def _():
                step_project(t - 0)

            @pl.when((t >= 1) & (t < micro))
            def _():
                step_weigh(t - 1)
                step_values(t - 1)

            @pl.when(t >= 2)
            def _():
                step_output(t - 2)

            @pl.when(t < micro)
            def _():
                step_scatter(t - 0)

            @pl.when((t >= group) & (t < micro))
            def _():
                step_gradient(t)

            @pl.when(t == micro - 1)
            def _():
                step_weigh(t)
                step_last_gradient()
                left_load.start()
                step_values(t)
                step_right()

            @pl.when((t >= 1) & (t < micro + 1))
            def _():
                step_forward(t - 1)


    @pl.when(s < last)
    def _():
        left_load.start()
        step_right()

    step_left()
    step_last_right()
    step_help()

    @pl.loop(0, micro)
    def _(m):
        wait_out(sq.at[m, pl.ds(0, dp - 1)], 1, m)
        wait_out(pair_send.at[m], 2, m)
        for owner in owners:
            @pl.when(z != owner)
            def _():
                wait_out(rs_send.at[m, 0], 3, m)

        @pl.when(is_owner)
        def _():
            wait_out(rs_recv.at[m], 4, m)

        wait_out(vals.at[m, c], 5, m)

        @pl.when(s < sections - 1)
        def _():
            wait_out(out.at[m], 0, m)


def relay(sections, dp, x_in, cot, gain, wv, wo, left, right):
    micro, rows_all, cols = x_in.shape
    width = wv.shape[1]
    chips = dp // 2
    half = rows_all // 2
    rows = half // len(owner_chips(chips))
    share = width // dp
    vmem = pl.BlockSpec(memory_space=pltpu.VMEM)
    anywhere = pl.BlockSpec(memory_space=pl.ANY)
    return pl.pallas_call(
        functools.partial(relay_kernel, sections, dp, cols * dp),
        out_shape=(
            pltpu.VMEM((micro, rows_all, cols), BF16),
            pltpu.VMEM((cols, width), F32),
            pltpu.VMEM((share, width), F32),
        ),
        in_specs=[anywhere, anywhere, vmem, anywhere, anywhere, anywhere, anywhere],
        out_specs=(vmem, vmem, vmem),
        scratch_shapes=[
            pltpu.VMEM((cols, width), BF16),
            pltpu.VMEM((micro, rows_all, cols), BF16),
            pltpu.VMEM((micro, rows_all, width), BF16),
            pltpu.VMEM((micro, rows_all, width), BF16),
            pltpu.VMEM((cols, width), BF16),
            pltpu.VMEM((width, cols), BF16),
            pltpu.VMEM((chips, 2, share, width), F32),
            pltpu.VMEM((chips, share, width), BF16),
            pltpu.VMEM((chips, share, width), BF16),
            pltpu.VMEM((chips - 1, share, width), BF16),
            pltpu.VMEM((chips - 1, share, width), BF16),
            pltpu.VMEM((chips - 1, share, width // 4), BF16),
            pltpu.VMEM((chips - 1, share, width // 4), BF16),
            pltpu.VMEM((share, width // 4), BF16),
            pltpu.VMEM((2, share, width // 4), BF16),
            pltpu.VMEM((micro, rows_all, cols), BF16),
            pltpu.VMEM((rows_all, width), F32),
            pltpu.VMEM((half, width), F32),
            pltpu.VMEM((rows_all, rows_all), F32),
            pltpu.VMEM((micro, dp, 8, rows_all), F32),
            pltpu.VMEM((micro, half, width), BF16),
            pltpu.VMEM((micro, half, width), BF16),
            pltpu.VMEM((micro, half // rows, rows, width), BF16),
            pltpu.VMEM((micro, chips - 1, rows, width), BF16),
            pltpu.VMEM((micro, 2, half // rows, rows, width), BF16),
            pltpu.SemaphoreType.DMA((6, micro)),
            pltpu.SemaphoreType.DMA((6, micro)),
            pltpu.SemaphoreType.DMA((PIECES, micro)),
            pltpu.SemaphoreType.DMA((5,)),
            pltpu.SemaphoreType.DMA((2, chips)),
            pltpu.SemaphoreType.DMA((2, chips - 1, 3)),
            pltpu.SemaphoreType.DMA((3, chips - 1)),
            pltpu.SemaphoreType.DMA((2, 2)),
        ],
        compiler_params=pltpu.CompilerParams(
            collective_id=0, has_side_effects=True, vmem_limit_bytes=VMEM_BYTES
        ),
    )(x_in, cot, gain, wv, wo, left, right)


def store_kernel(out, left, right, out_hbm, left_hbm, right_hbm, sem):
    copies = [
        pltpu.make_async_copy(src, dst, sem.at[i])
        for i, (src, dst) in enumerate(((left, left_hbm), (out, out_hbm), (right, right_hbm)))
    ]
    for copy in copies:
        copy.start()
    for copy in copies:
        copy.wait()


def store(*arrays):
    vmem = pl.BlockSpec(memory_space=pltpu.VMEM)
    anywhere = pl.BlockSpec(memory_space=pl.ANY)
    return pl.pallas_call(
        store_kernel,
        out_shape=tuple(jax.ShapeDtypeStruct(a.shape, a.dtype) for a in arrays),
        in_specs=[vmem] * 3,
        out_specs=(anywhere,) * 3,
        scratch_shapes=[pltpu.SemaphoreType.DMA((3,))],
        compiler_params=pltpu.CompilerParams(vmem_limit_bytes=1024 * 1024),
    )(*[pltpu.with_memory_space_constraint(a, pltpu.VMEM) for a in arrays])


def on_device(inputs, cotangent, norm_gain, value_weight, output_weight, left_old, right_old):
    sections = lax.axis_size("section")
    dp = lax.axis_size("dp")
    micro, rows_all, cols = inputs.shape
    width = value_weight.shape[2]
    chips = dp // 2
    split = 2 if rows_all // dp >= 16 else 1
    chunked = (micro * split, rows_all // split)
    outputs, left_new, right_new = store(*relay(
        sections, dp, inputs.reshape(chunked + (cols,)), cotangent[0].reshape(chunked + (width,)),
        norm_gain, value_weight[0], output_weight[0], left_old.reshape(cols, width), right_old[0],
    ))
    outputs = outputs.reshape((1, micro, rows_all, cols))
    return (outputs, left_new.reshape(left_old.shape), right_new[None])


def solution(mesh):
    placed = (
        P(None, None, "dp"),
        P("section", None, None, None),
        P("section", "dp"),
        P("section", "dp", None),
        P("section", None, "dp"),
        P("section", "dp", None, None),
        P("section", "dp", None),
    )
    return jax.shard_map(
        on_device,
        mesh=mesh,
        in_specs=placed,
        out_specs=(
            P("section", None, None, "dp"),
            P("section", "dp", None, None),
            P("section", "dp", None),
        ),
        check_vma=False,
    )
```

```python
import functools

import jax
import jax.numpy as jnp
from jax import lax
from jax.experimental import pallas as pl
from jax.experimental.pallas import tpu as pltpu
from jax.sharding import PartitionSpec as P

BLOCK = 1024
PIECES = 4
VMEM_BYTES = 46 * 1024 * 1024
MESH = pl.DeviceIdType.MESH
F32 = jnp.float32
BF16 = jnp.bfloat16


def owner_chips(chips):
    return (chips // 2 - 1, chips // 2) if chips >= 4 else tuple(range(chips))


def relay_kernel(
    sections, dp, model_width,
    x_in, cot_in, gain, wv_in, wo_in, left_in, right_in,
    out, acc, right_out,
    grad, scaled, weighted, cot, wv, wo, right_own, right_send, right_recv,
    z_send, z_recv, help_in, help_recv, help_send, help_back,
    xbuf, prod, csum, invs, sq, pair_send, pair_recv, rs_send, rs_recv, vals,
    send_sem, recv_sem, x_sem, load_sem, right_sem, z_sem, help_sem, back_sem,
):
    chips = dp // 2
    micro, rows_all, cols = x_in.shape
    width = wv.shape[1]
    half = rows_all // 2
    owners = owner_chips(chips)
    rows = half // len(owners)
    share = width // dp
    s = lax.axis_index("section")
    d = lax.axis_index("dp")
    z = d // 2
    c = lax.rem(d, 2)
    partner = z * 2 + (1 - c)
    last = sections - 1
    helpers = (last ^ 2, last ^ 3) if sections % 4 == 0 else ()
    own_cols = 5 * width // 8 if helpers else width
    slices = (width // 4, width // 8)

    def device(section, index):
        return (section, index)

    piece = cols // PIECES

    def load_x(m):
        for p in range(PIECES):
            lanes = pl.ds(p * piece, piece)
            pltpu.make_async_copy(
                x_in.at[m, :, lanes], xbuf.at[m, :, lanes], x_sem.at[p, m]
            ).start()

    loads = [
        pltpu.make_async_copy(src, dst, load_sem.at[i])
        for i, (src, dst) in enumerate(((wv_in, wv), (cot_in, cot), (wo_in, wo), (right_in, right_out)))
    ]
    left_load = pltpu.make_async_copy(left_in, acc, load_sem.at[4])

    @pl.when(s == 0)
    def _():
        load_x(0)

    loads[0].start()

    @pl.when(s == 0)
    def _():
        @pl.loop(1, micro)
        def _(m):
            load_x(m)

    barrier = pltpu.get_barrier_semaphore()
    for j in range(1, dp):
        pl.semaphore_signal(barrier, inc=1, device_id=device(s, lax.rem(d + j, dp)), device_id_type=MESH)

    @pl.when(s > 0)
    def _():
        pl.semaphore_signal(barrier, inc=1, device_id=device(s - 1, d), device_id_type=MESH)

    @pl.when(s < sections - 1)
    def _():
        pl.semaphore_signal(barrier, inc=1, device_id=device(s + 1, d), device_id_type=MESH)

    greeted = dp - 1 + jnp.minimum(s, 1) + jnp.minimum(sections - 1 - s, 1)
    for h in helpers:
        for there, here in ((last, h), (h, last)):
            @pl.when(s == here)
            def _():
                pl.semaphore_signal(barrier, inc=1, device_id=device(there, d), device_id_type=MESH)

            greeted = greeted + jnp.where(s == here, 1, 0)

    pl.semaphore_wait(barrier, greeted)

    def send(src, dst, phase, m, section, index):
        pltpu.make_async_remote_copy(
            src_ref=src, dst_ref=dst,
            send_sem=send_sem.at[phase, m], recv_sem=recv_sem.at[phase, m],
            device_id=device(section, index), device_id_type=MESH,
        ).start()

    def wait_in(ref, phase, m):
        pltpu.make_async_copy(ref, ref, recv_sem.at[phase, m]).wait()

    def wait_out(ref, phase, m):
        pltpu.make_async_copy(ref, ref, send_sem.at[phase, m]).wait()

    def step_project(m):
        total = jnp.zeros((rows_all, 128), F32)
        for p in range(PIECES):
            lanes = pl.ds(p * piece, piece)
            ref = xbuf.at[m, :, lanes]
            pltpu.make_async_copy(ref, ref, x_sem.at[p, m]).wait()
            for k in range(p * piece // 128, (p + 1) * piece // 128):
                values = xbuf[m, :, k * 128:(k + 1) * 128].astype(F32)
                total = total + values * values
                scaled[m, :, k * 128:(k + 1) * 128] = (
                    values * gain[:, k * 128:(k + 1) * 128].astype(F32)
                ).astype(BF16)
            if p == PIECES - 1:
                row = jnp.sum(total.T, axis=0, keepdims=True)
                sq[m, d] = jnp.broadcast_to(row, (8, rows_all))
                for j in range(1, dp):
                    send(sq.at[m, d], sq.at[m, d], 1, m, s, lax.rem(d + j, dp))
            if p == 0:
                @pl.when(m == 0)
                def _():
                    loads[0].wait()
                    for load in loads[1:]:
                        load.start()
            product = jnp.dot(scaled[m, :, lanes], wv[lanes, :], preferred_element_type=F32)
            if p == 0:
                prod[...] = product
            else:
                prod[...] += product

        pair_send[m] = prod[pl.ds(pl.multiple_of((1 - c) * half, half), half), :].astype(BF16)
        send(pair_send.at[m], pair_recv.at[m], 2, m, s, partner)

    is_owner = functools.reduce(jnp.logical_or, [z == owner for owner in owners])

    def wait_values(wait, m):
        @pl.when(is_owner)
        def _():
            if len(owners) > 1:
                wait(vals.at[m, c, pl.ds(0, len(owners) - 1)], 4, m)

        @pl.when(jnp.logical_not(is_owner))
        def _():
            wait(vals.at[m, c], 4, m)

    def step_forward(m):
        wait_values(wait_in, m)
        send(vals.at[m, c], vals.at[m, c], 5, m, s, partner)

    def step_scatter(m):
        wait_in(pair_recv.at[m], 2, m)
        csum[...] = prod[pl.ds(pl.multiple_of(c * half, half), half), :] + pair_recv[m].astype(F32)
        for i, owner in enumerate(owners):
            @pl.when(z != owner)
            def _():
                rs_send[m, i] = csum[i * rows:(i + 1) * rows, :].astype(BF16)
                slot = lax.rem(z - owner + chips, chips) - 1
                send(rs_send.at[m, i], rs_recv.at[m, slot], 3, m, s, owner * 2 + c)

    def step_output(m):
        wait_in(vals.at[m, 1 - c], 5, m)

        @pl.when(m == 0)
        def _():
            loads[2].wait()

        values = vals[m].reshape(rows_all, width)

        for p in range(PIECES):
            lanes = pl.ds(p * piece, piece)
            out[m, :, lanes] = (
                xbuf[m, :, lanes].astype(F32)
                + jnp.dot(values, wo[:, lanes], preferred_element_type=F32)
            ).astype(BF16)

            @pl.when(s < sections - 1)
            def _():
                pltpu.make_async_remote_copy(
                    src_ref=out.at[m, :, lanes], dst_ref=xbuf.at[m, :, lanes],
                    send_sem=send_sem.at[0, m], recv_sem=x_sem.at[p, m],
                    device_id=device(s + 1, d), device_id_type=MESH,
                ).start()

    def step_weigh(m):
        wait_in(sq.at[m, pl.ds(0, dp - 1)], 1, m)
        total_sq = jnp.sum(sq[m], axis=0)
        inv = lax.rsqrt(total_sq / model_width + 0.25)
        invs[...] = jnp.broadcast_to(inv[0:1, :], (rows_all, rows_all)).T

        @pl.when(m == 0)
        def _():
            loads[1].wait()

        weighted[m] = (invs[:, 0:1] * cot[m].astype(F32)).astype(BF16)

    def step_values(m):
        for i, owner in enumerate(owners):
            @pl.when(z == owner)
            def _():
                wait_in(rs_recv.at[m], 3, m)
                total = csum[i * rows:(i + 1) * rows, :]
                for j in range(chips - 1):
                    total = total + rs_recv[m, j].astype(F32)
                own = invs[pl.ds(pl.multiple_of(c * half + i * rows, rows), rows), 0:1]
                vals[m, c, i] = (own * total).astype(BF16)
                for j in range(1, chips):
                    target = (owner + j) % chips
                    send(vals.at[m, c, i], vals.at[m, c, i], 4, m, s, target * 2 + c)

    contract_rows = (((0,), (0,)), ((), ()))
    group = max(1, 256 // rows_all)
    groups = micro // group

    def gradient_tile(pair, n, tile):
        at = pl.ds(pl.multiple_of(n * tile, tile), tile)
        left = scaled[pl.ds(pair * group, group), :, at].reshape(group * rows_all, tile)
        right = weighted[pl.ds(pair * group, group)].reshape(group * rows_all, width)
        return at, lax.dot_general(left, right, contract_rows, preferred_element_type=F32)

    def step_gradient(t):
        pair = (t - group) // group
        at, update = gradient_tile(pair, lax.rem(t, group), cols // group)

        @pl.when(pair == 0)
        def _():
            acc[at, :] = update

        @pl.when(pair > 0)
        def _():
            acc[at, :] += update

    def step_last_gradient():
        tile = cols // 2

        @pl.loop(0, 2)
        def _(n):
            at, update = gradient_tile(groups - 1, n, tile)
            grad[at, :] = (acc[at, :] + update).astype(BF16)

    def right_product(j):
        target = lax.rem(z + j, chips)
        at = pl.ds(pl.multiple_of(target * 2 * share, 2 * share), 2 * share)

        product = lax.dot_general(
            grad[:, at], grad[...], contract_rows, preferred_element_type=F32
        )
        right_own[j] = product.reshape(2, share, width)
        right_send[j] = right_own[j, 1 - c].astype(BF16)
        pltpu.make_async_remote_copy(
            src_ref=right_send.at[j], dst_ref=right_recv.at[j],
            send_sem=right_sem.at[0, j], recv_sem=right_sem.at[1, j],
            device_id=device(s, partner), device_id_type=MESH,
        ).start()

    def right_scatter(j):
        pltpu.make_async_copy(right_recv.at[j], right_recv.at[j], right_sem.at[1, j]).wait()
        z_send[j - 1] = (right_own[j, c] + right_recv[j].astype(F32)).astype(BF16)
        target = lax.rem(z + j, chips) * 2 + c
        slot = chips - 1 - j

        def scatter(cut, dst, part, recv, section, target=target):
            pltpu.make_async_remote_copy(
                src_ref=z_send.at[j - 1, :, cut], dst_ref=dst,
                send_sem=z_sem.at[0, j - 1, part], recv_sem=recv,
                device_id=device(section, target), device_id_type=MESH,
            ).start()

        own = pl.ds(0, own_cols)
        scatter(own, z_recv.at[slot, :, own], 0, z_sem.at[1, slot, 0], s)
        for i, h in enumerate(helpers):
            cut = pl.ds(own_cols + sum(slices[:i]), slices[i])

            @pl.when(s == last)
            def _():
                scatter(cut, help_in.at[j - 1, :, pl.ds(0, slices[i])], 1 + i, help_sem.at[0, j - 1], h, d)

            @pl.when(s < last)
            def _():
                scatter(cut, z_recv.at[slot, :, cut], 1 + i, z_sem.at[1, slot, 1 + i], s)

    def step_right():
        for j in range(1, chips):
            right_product(j)
            if j > 1:
                right_scatter(j - 1)
        right_product(0)
        right_scatter(chips - 1)

    def step_left():
        left_load.wait()
        for block in range(cols // BLOCK):
            @pl.loop(0, BLOCK // 512)
            def _(n):
                at = pl.ds(pl.multiple_of(block * BLOCK + n * 512, 512), 512)
                product = lax.dot_general(
                    grad[at, :], grad[block * BLOCK:(block + 1) * BLOCK, :],
                    (((1,), (1,)), ((), ())), preferred_element_type=F32,
                )
                acc[at, :] += product * (1.0 / BLOCK)

    def step_last_right():
        pltpu.make_async_copy(right_recv.at[0], right_recv.at[0], right_sem.at[1, 0]).wait()
        loads[3].wait()
        scale = 1.0 / model_width

        def gather(cut, part):
            total = right_own[0, c, :, cut] + right_recv[0, :, cut].astype(F32)
            for k in range(chips - 1):
                ref = z_recv.at[k, :, cut]
                pltpu.make_async_copy(ref, ref, z_sem.at[1, k, part]).wait()
                total = total + z_recv[k, :, cut].astype(F32)
            right_out[:, cut] += total * scale

        gather(pl.ds(0, own_cols), 0)
        for i, h in enumerate(helpers):
            cut = pl.ds(own_cols + sum(slices[:i]), slices[i])

            @pl.when(s == last)
            def _():
                ref = help_back.at[i, :, pl.ds(0, slices[i])]
                pltpu.make_async_copy(ref, ref, back_sem.at[1, i]).wait()
                total = right_own[0, c, :, cut] + right_recv[0, :, cut].astype(F32)
                right_out[:, cut] += (total + help_back[i, :, :slices[i]].astype(F32)) * scale

            @pl.when(s < last)
            def _():
                gather(cut, 1 + i)

        for j in range(chips):
            pltpu.make_async_copy(right_send.at[j], right_send.at[j], right_sem.at[0, j]).wait()
        for j in range(chips - 1):
            for part in range(1 + len(helpers)):
                ref = z_send.at[j, :, pl.ds(0, slices[part - 1] if part else own_cols)]
                pltpu.make_async_copy(ref, ref, z_sem.at[0, j, part]).wait()

    def step_help():
        for i, h in enumerate(helpers):
            @pl.when(s == h)
            def _():
                for j in range(1, chips):
                    ref = help_in.at[j - 1, :, pl.ds(0, slices[i])]
                    pltpu.make_async_copy(ref, ref, help_sem.at[0, j - 1]).wait()
                    pltpu.make_async_remote_copy(
                        src_ref=ref, dst_ref=help_recv.at[chips - 1 - j, :, pl.ds(0, slices[i])],
                        send_sem=help_sem.at[2, j - 1], recv_sem=help_sem.at[1, chips - 1 - j],
                        device_id=device(s, lax.rem(z + j, chips) * 2 + c), device_id_type=MESH,
                    ).start()
                total = None
                for k in range(chips - 1):
                    ref = help_recv.at[k, :, pl.ds(0, slices[i])]
                    pltpu.make_async_copy(ref, ref, help_sem.at[1, k]).wait()
                    piece = help_recv[k, :, :slices[i]].astype(F32)
                    total = piece if total is None else total + piece
                help_send[:, :slices[i]] = total.astype(BF16)
                back = pltpu.make_async_remote_copy(
                    src_ref=help_send.at[:, pl.ds(0, slices[i])],
                    dst_ref=help_back.at[i, :, pl.ds(0, slices[i])],
                    send_sem=back_sem.at[0, i], recv_sem=back_sem.at[1, i],
                    device_id=device(last, d), device_id_type=MESH,
                )
                back.start()
                for k in range(chips - 1):
                    ref = help_in.at[k, :, pl.ds(0, slices[i])]
                    pltpu.make_async_copy(ref, ref, help_sem.at[2, k]).wait()
                back.wait_send()

    @pl.when(s == 0)
    def _():
        @pl.loop(0, micro + 2)
        def _(t):
            @pl.when(t < micro)
            def _():
                step_project(t - 0)

            @pl.when(t >= 2)
            def _():
                step_forward(t - 2)

            @pl.when((t >= 1) & (t < micro + 1))
            def _():
                step_weigh(t - 1)

            @pl.when((t >= 1) & (t < micro + 1))
            def _():
                step_values(t - 1)

            @pl.when((t >= group) & (t < micro))
            def _():
                step_gradient(t)

            @pl.when(t == micro)
            def _():
                step_last_gradient()

            @pl.when(t < micro)
            def _():
                step_scatter(t - 0)

            @pl.when(t >= 2)
            def _():
                step_output(t - 2)


    @pl.when((s > 0) & (s < last))
    def _():
        @pl.loop(0, micro + 2)
        def _(t):
            @pl.when(t < micro)
            def _():
                step_project(t - 0)

            @pl.when((t >= 1) & (t < micro + 1))
            def _():
                step_weigh(t - 1)

            @pl.when((t >= 1) & (t < micro + 1))
            def _():
                step_values(t - 1)

            @pl.when(t >= 2)
            def _():
                step_output(t - 2)

            @pl.when(t < micro)
            def _():
                step_scatter(t - 0)

            @pl.when((t >= group) & (t < micro))
            def _():
                step_gradient(t)

            @pl.when(t == micro)
            def _():
                step_last_gradient()

            @pl.when((t >= 1) & (t < micro + 1))
            def _():
                step_forward(t - 1)


    @pl.when(s == last)
    def _():
        @pl.loop(0, micro + 2)
        def _(t):
            @pl.when(t < micro)
            def _():
                step_project(t - 0)

            @pl.when((t >= 1) & (t < micro))
            def _():
                step_weigh(t - 1)
                step_values(t - 1)

            @pl.when(t >= 2)
            def _():
                step_output(t - 2)

            @pl.when(t < micro)
            def _():
                step_scatter(t - 0)

            @pl.when((t >= group) & (t < micro))
            def _():
                step_gradient(t)

            @pl.when(t == micro - 1)
            def _():
                step_weigh(t)
                step_last_gradient()
                left_load.start()
                step_values(t)
                step_right()

            @pl.when((t >= 1) & (t < micro + 1))
            def _():
                step_forward(t - 1)


    @pl.when(s < last)
    def _():
        left_load.start()
        step_right()

    step_left()
    step_last_right()
    step_help()

    @pl.loop(0, micro)
    def _(m):
        wait_out(sq.at[m, pl.ds(0, dp - 1)], 1, m)
        wait_out(pair_send.at[m], 2, m)
        for owner in owners:
            @pl.when(z != owner)
            def _():
                wait_out(rs_send.at[m, 0], 3, m)

        @pl.when(is_owner)
        def _():
            wait_out(rs_recv.at[m], 4, m)

        wait_out(vals.at[m, c], 5, m)

        @pl.when(s < sections - 1)
        def _():
            wait_out(out.at[m], 0, m)


def relay(sections, dp, x_in, cot, gain, wv, wo, left, right):
    micro, rows_all, cols = x_in.shape
    width = wv.shape[1]
    chips = dp // 2
    half = rows_all // 2
    rows = half // len(owner_chips(chips))
    share = width // dp
    vmem = pl.BlockSpec(memory_space=pltpu.VMEM)
    anywhere = pl.BlockSpec(memory_space=pl.ANY)
    return pl.pallas_call(
        functools.partial(relay_kernel, sections, dp, cols * dp),
        out_shape=(
            pltpu.VMEM((micro, rows_all, cols), BF16),
            pltpu.VMEM((cols, width), F32),
            pltpu.VMEM((share, width), F32),
        ),
        in_specs=[anywhere, anywhere, vmem, anywhere, anywhere, anywhere, anywhere],
        out_specs=(vmem, vmem, vmem),
        scratch_shapes=[
            pltpu.VMEM((cols, width), BF16),
            pltpu.VMEM((micro, rows_all, cols), BF16),
            pltpu.VMEM((micro, rows_all, width), BF16),
            pltpu.VMEM((micro, rows_all, width), BF16),
            pltpu.VMEM((cols, width), BF16),
            pltpu.VMEM((width, cols), BF16),
            pltpu.VMEM((chips, 2, share, width), F32),
            pltpu.VMEM((chips, share, width), BF16),
            pltpu.VMEM((chips, share, width), BF16),
            pltpu.VMEM((chips - 1, share, width), BF16),
            pltpu.VMEM((chips - 1, share, width), BF16),
            pltpu.VMEM((chips - 1, share, width // 4), BF16),
            pltpu.VMEM((chips - 1, share, width // 4), BF16),
            pltpu.VMEM((share, width // 4), BF16),
            pltpu.VMEM((2, share, width // 4), BF16),
            pltpu.VMEM((micro, rows_all, cols), BF16),
            pltpu.VMEM((rows_all, width), F32),
            pltpu.VMEM((half, width), F32),
            pltpu.VMEM((rows_all, rows_all), F32),
            pltpu.VMEM((micro, dp, 8, rows_all), F32),
            pltpu.VMEM((micro, half, width), BF16),
            pltpu.VMEM((micro, half, width), BF16),
            pltpu.VMEM((micro, half // rows, rows, width), BF16),
            pltpu.VMEM((micro, chips - 1, rows, width), BF16),
            pltpu.VMEM((micro, 2, half // rows, rows, width), BF16),
            pltpu.SemaphoreType.DMA((6, micro)),
            pltpu.SemaphoreType.DMA((6, micro)),
            pltpu.SemaphoreType.DMA((PIECES, micro)),
            pltpu.SemaphoreType.DMA((5,)),
            pltpu.SemaphoreType.DMA((2, chips)),
            pltpu.SemaphoreType.DMA((2, chips - 1, 3)),
            pltpu.SemaphoreType.DMA((3, chips - 1)),
            pltpu.SemaphoreType.DMA((2, 2)),
        ],
        compiler_params=pltpu.CompilerParams(
            collective_id=0, has_side_effects=True, vmem_limit_bytes=VMEM_BYTES
        ),
    )(x_in, cot, gain, wv, wo, left, right)


def store_kernel(out, left, right, out_hbm, left_hbm, right_hbm, sem):
    copies = [
        pltpu.make_async_copy(src, dst, sem.at[i])
        for i, (src, dst) in enumerate(((left, left_hbm), (out, out_hbm), (right, right_hbm)))
    ]
    for copy in copies:
        copy.start()
    for copy in copies:
        copy.wait()


def store(*arrays):
    vmem = pl.BlockSpec(memory_space=pltpu.VMEM)
    anywhere = pl.BlockSpec(memory_space=pl.ANY)
    return pl.pallas_call(
        store_kernel,
        out_shape=tuple(jax.ShapeDtypeStruct(a.shape, a.dtype) for a in arrays),
        in_specs=[vmem] * 3,
        out_specs=(anywhere,) * 3,
        scratch_shapes=[pltpu.SemaphoreType.DMA((3,))],
        compiler_params=pltpu.CompilerParams(vmem_limit_bytes=1024 * 1024),
    )(*[pltpu.with_memory_space_constraint(a, pltpu.VMEM) for a in arrays])


def on_device(inputs, cotangent, norm_gain, value_weight, output_weight, left_old, right_old):
    sections = lax.axis_size("section")
    dp = lax.axis_size("dp")
    micro, rows_all, cols = inputs.shape
    width = value_weight.shape[2]
    chips = dp // 2
    split = 2 if rows_all // dp >= 16 else 1
    chunked = (micro * split, rows_all // split)
    outputs, left_new, right_new = store(*relay(
        sections, dp, inputs.reshape(chunked + (cols,)), cotangent[0].reshape(chunked + (width,)),
        norm_gain, value_weight[0], output_weight[0], left_old.reshape(cols, width), right_old[0],
    ))
    outputs = outputs.reshape((1, micro, rows_all, cols))
    return (outputs, left_new.reshape(left_old.shape), right_new[None])


def solution(mesh):
    placed = (
        P(None, None, "dp"),
        P("section", None, None, None),
        P("section", "dp"),
        P("section", "dp", None),
        P("section", None, "dp"),
        P("section", "dp", None, None),
        P("section", "dp", None),
    )
    return jax.shard_map(
        on_device,
        mesh=mesh,
        in_specs=placed,
        out_specs=(
            P("section", None, None, "dp"),
            P("section", "dp", None, None),
            P("section", "dp", None),
        ),
        check_vma=False,
    )
```
